32 devices in a mesh: groups: 2 (over y), wide: 4 (over z), narrow: 4 (over x, core).
Axes of the slice: x: 2, y: 2, z: 4, core: 2. Of those that a mesh axis runs over, the one named last changes fastest.
Arguments:
- cont_queries: bfloat16 [32, 128, 64, 128], P(('groups', 'wide'), None, 'narrow'), parts along dimension 0, may hold values from -5 to 5
- cont_keys: bfloat16 [32, 128, 8, 128], P(('groups', 'wide'), None, 'narrow'), parts along dimension 0, may hold values from -5 to 5
- cont_values: bfloat16 [32, 128, 8, 128], P(('groups', 'wide'), None, 'narrow'), parts along dimension 0, may hold values from -5 to 5
- prefix_kv: bfloat16 [8, 2, 128, 8, 128], P(('groups', 'wide'), None, None, 'narrow'), parts along dimension 0, may hold values from -5 to 5
- probe: bfloat16 [64, 128], P('narrow'), may hold values from -0.5 to 0.5
- question_row: int32 [8], P('groups'), parts along dimension 0, may hold values from 0 to 3, each once
- cont_slot: int32 [32], P(('groups', 'wide')), parts along dimension 0, may hold values from 0 to 15, each once
- cont_length: int32 [32], P(('groups', 'wide')), parts along dimension 0, may hold values from 1 to 128
- gold: int32 [8], P('groups'), parts along dimension 0, may hold values from 0 to 3
Outputs:
- token_score: float32 [32, 128], P(('groups', 'wide')), parts along dimension 0
- owned_logprob: float32 [8, 4], P(('groups', 'wide')), parts along dimension 0
- owned_loss: float32 [8], P(('groups', 'wide')), parts along dimension 0
The draws below stay inside these ranges and needn't reach their ends.
There are 2 independent parts, one for each index of `groups`. The reference program is written for one: setup_inputs(seed, part) draws one part's arguments, and reference() takes and returns one part's arrays. A program takes and returns all parts, laid end to end along the dimension named above; an argument that names none is the same for every part. Nothing has to cross between parts.
All inputs are finite; a program needn't handle non-finite values.
Results may differ from the reference program's by a relative error of at most 0.0065.
Values may be sent and summed in bfloat16 or wider, within the bound.
No kernel may reach another device: no remote copies, remote signals or barrier semaphores. Data moves between devices by JAX's collectives and lax.ppermute only.
A program may use at most 64 MiB of HBM per device.

```python
import jax
import jax.numpy as jnp
from jax import lax

HEADS = 64
KV_HEADS = 8
HEAD_DIM = 128
ANSWERS = 4
CLEN = 128
PREF = 128
QUESTIONS = 4
CONTS = 16


def draw_cont_queries(key, part):
    drawn = jax.random.normal(jax.random.fold_in(key, 1), (CONTS, CLEN, HEADS, HEAD_DIM), jnp.float32)
    drawn = jnp.clip(drawn, -5.0, 5.0)
    return drawn.astype(jnp.bfloat16)


def draw_prefix_kv(key, part):
    drawn = jax.random.normal(jax.random.fold_in(key, 2), (QUESTIONS, 2, PREF, KV_HEADS, HEAD_DIM), jnp.float32)
    drawn = jnp.clip(drawn, -5.0, 5.0)
    return drawn.astype(jnp.bfloat16)


def plant(values, rng, least, top_value):
    dims = values.shape
    index_at = [jax.random.randint(jax.random.fold_in(rng, axis), (), 0, dims[axis]) for axis in range(len(dims))]
    values = values.at[tuple(index_at)].set(least)
    longest = dims.index(max(dims))
    index_at[longest] = (index_at[longest] + 1) % dims[longest]
    return values.at[tuple(index_at)].set(top_value)


def steps_of(own_key, dims, cuts, low, top_value):
    gain = 1.0
    for dim, blocks in cuts:
        steps = jax.random.uniform(jax.random.fold_in(jax.random.fold_in(own_key, 6), dim), (blocks,), jnp.float32, low / len(cuts), top_value / len(cuts))
        gain = gain * jnp.repeat(jnp.exp(steps), dims[dim] // blocks).reshape((-1,) + (1,) * (len(dims) - 1 - dim))
    return gain


def noise(own_key, shape, spread, limit, split=(), held_as=jnp.bfloat16):
    result = jax.random.normal(own_key, shape, jnp.float32) * spread
    if len(split) > 0:
        result = steps_of(own_key, shape, split, -0.22, 0.18) * result
    return jnp.clip(result, min=-limit, max=limit).astype(held_as)


def setup_inputs(seed: int = 0, part: int = 0) -> dict:
    key_list = jax.random.split(jax.random.key(seed), 10)
    own_keys = jax.random.split(jax.random.fold_in(key_list[9], part), 10)
    return {
        "cont_queries": draw_cont_queries(jax.random.fold_in(jax.random.fold_in(key_list[9], part), 71), part),
        "cont_keys": noise(own_keys[1], (CONTS, CLEN, KV_HEADS, HEAD_DIM), 1.0, 5.0, ((0, 4), (2, 4))),
        "cont_values": noise(own_keys[2], (CONTS, CLEN, KV_HEADS, HEAD_DIM), 1.0, 5.0, ((0, 4), (2, 4))),
        "prefix_kv": draw_prefix_kv(jax.random.fold_in(jax.random.fold_in(key_list[9], part), 71), part),
        "probe": noise(key_list[4], (HEADS, HEAD_DIM), HEAD_DIM ** -0.5, 0.5, ((0, 4),)),
        "question_row": jax.random.permutation(own_keys[5], QUESTIONS).astype(jnp.int32),
        "cont_slot": jax.random.permutation(own_keys[6], CONTS).astype(jnp.int32),
        "cont_length": plant(jax.random.randint(own_keys[7], (CONTS,), 1, CLEN + 1), jax.random.fold_in(own_keys[7], 1), 1, CLEN).astype(jnp.int32),
        "gold": plant(jax.random.randint(own_keys[8], (QUESTIONS,), 0, ANSWERS), jax.random.fold_in(own_keys[8], 1), 0, ANSWERS - 1).astype(jnp.int32),
    }


def reference(cont_queries, cont_keys, cont_values, prefix_kv, probe, question_row, cont_slot, cont_length, gold):
    group_size = HEADS // KV_HEADS
    scale_factor = 1.0 / (HEAD_DIM ** 0.5)
    wanted = question_row[cont_slot // ANSWERS].astype(jnp.int32)
    causal = jnp.arange(CLEN)[:, None] >= jnp.arange(CLEN)[None, :]
    allowed = jnp.concatenate([jnp.ones((CLEN, PREF), dtype=bool), causal], axis=1)

    def score_one(packed):
        queries, keys_own, values_own, prefix_row = packed
        cached = lax.dynamic_index_in_dim(prefix_kv, prefix_row, 0, keepdims=False)
        keys_all = jnp.concatenate([cached[0], keys_own], axis=0)
        values_all = jnp.concatenate([cached[1], values_own], axis=0)
        keys_wide = jnp.repeat(keys_all, group_size, axis=1).astype(jnp.float32)
        values_wide = jnp.repeat(values_all, group_size, axis=1).astype(jnp.float32)
        scores = jnp.einsum("thd,jhd->htj", queries.astype(jnp.float32), keys_wide) * scale_factor
        scores = jnp.where(allowed[None, :, :], scores, -jnp.inf)
        row_max = jnp.max(scores, axis=-1, keepdims=True)
        expo = jnp.exp(scores - row_max)
        total = jnp.sum(expo, axis=-1)
        weights = expo.astype(jnp.bfloat16)
        summed = jnp.einsum("htj,jhd->thd", weights.astype(jnp.float32), values_wide)
        attended = (summed / jnp.transpose(total)[:, :, None]).astype(jnp.bfloat16)
        return jnp.einsum("thd,hd->t", attended.astype(jnp.float32), probe.astype(jnp.float32))

    token_score = lax.map(score_one, (cont_queries, cont_keys, cont_values, wanted))
    valid = jnp.arange(CLEN)[None, :] < cont_length[:, None]
    choice_score = jnp.sum(jnp.where(valid, token_score, jnp.zeros_like(token_score)), axis=1)
    question_score = jnp.zeros((QUESTIONS * ANSWERS,), jnp.float32).astype(choice_score.dtype)
    question_score = question_score.at[cont_slot].set(choice_score).reshape(QUESTIONS, ANSWERS)
    logprob = question_score - jax.nn.logsumexp(question_score, axis=1, keepdims=True)
    owned_logprob = jnp.zeros_like(logprob).at[question_row].set(logprob)
    picked = jnp.take_along_axis(logprob, gold[:, None].astype(jnp.int32), axis=1)[:, 0]
    owned_loss = jnp.zeros_like(picked).at[question_row].set(-picked)
    return token_score, owned_logprob, owned_loss
```

```python
import math

import jax
import jax.numpy as jnp
from jax import lax
from jax.experimental import pallas as pl
from jax.experimental.pallas import tpu as pltpu
from jax.sharding import PartitionSpec as P

ANSWERS = 4
DIRECT_LIMIT = 8
F32 = jnp.float32
BF16 = jnp.bfloat16


def dot_nt(a, b):
    return lax.dot_general(a, b, (((1,), (1,)), ((), ())), preferred_element_type=F32)


def dot_tn(a, b):
    return lax.dot_general(a, b, (((0,), (0,)), ((), ())), preferred_element_type=F32)


def column_chunk(clen, group_size):
    cols = clen * group_size
    return 256 if cols % 256 == 0 else cols


def pack_kernel(prefix_ref, probe_ref, out_ref):
    pref_len, kv_here, head_dim = prefix_ref.shape[2:]
    heads_here = probe_ref.shape[0]
    group = heads_here // kv_here
    reads = []
    for k in range(kv_here):
        out_ref[0, k * pref_len : (k + 1) * pref_len, :] = prefix_ref[0, 0, :, k, :]
        reads.append(dot_nt(probe_ref[k * group : (k + 1) * group, :], prefix_ref[0, 1, :, k, :]))
    read = jnp.concatenate(reads, axis=0)
    high = read.astype(BF16)
    low = (read - high.astype(F32)).astype(BF16)
    base = kv_here * pref_len
    out_ref[0, base : base + heads_here, :] = high
    out_ref[0, base + heads_here : base + 2 * heads_here, :] = low


def own_kernel(query_ref, key_ref, value_ref, probe_ref, stat_ref):
    clen, kv_here, head_dim = key_ref.shape[1:]
    group = query_ref.shape[2] // kv_here
    cols = clen * group
    chunk = column_chunk(clen, group)
    span = chunk // group
    factor = math.log2(math.e) / math.sqrt(head_dim)
    row = lax.broadcasted_iota(jnp.int32, (span, chunk), 0)
    col = lax.broadcasted_iota(jnp.int32, (span, chunk), 1)
    seen = row * group <= col
    for k in range(kv_here):
        keys = key_ref[0, :, k, :]
        probe = probe_ref[k * group : (k + 1) * group, :]
        read = dot_nt(value_ref[0, :, k, :], jnp.concatenate([probe] * (chunk // group), axis=0))
        for start in range(0, cols, chunk):
            first = start // group
            last = first + span
            query = query_ref[0, first:last, k * group : (k + 1) * group, :].reshape(chunk, head_dim)
            scores = dot_nt(keys[:last], query)
            edge = jnp.where(seen, scores[first:last], -jnp.inf)
            scores = edge if first == 0 else jnp.concatenate([scores[:first], edge], axis=0)
            top = jnp.max(scores, axis=0, keepdims=True)
            expo = jnp.exp2((scores - top) * factor)
            total = jnp.sum(expo, axis=0, keepdims=True)
            summed = jnp.sum(expo * read[:last], axis=0, keepdims=True)
            stat_ref[0, 3 * k : 3 * k + 1, start : start + chunk] = top
            stat_ref[0, 3 * k + 1 : 3 * k + 2, start : start + chunk] = total
            stat_ref[0, 3 * k + 2 : 3 * k + 3, start : start + chunk] = summed


def prefix_kernel(source_ref, place_ref, target_ref, length_ref, query_ref, stat_ref, *rest, sources):
    piece_refs = rest[:sources]
    out_ref, cache, outcome, sem = rest[sources:]
    cont_count = cache.shape[0]
    c = pl.program_id(0)
    clen, heads_here, head_dim = query_ref.shape[1:]
    kv_here = stat_ref.shape[1] // 3
    group = heads_here // kv_here
    cols = clen * group
    chunk = column_chunk(clen, group)
    span = chunk // group
    pref_len = (cache.shape[1] - 2 * heads_here) // kv_here
    factor = math.log2(math.e) / math.sqrt(head_dim)

    @pl.when(c == 0)
    def _():
        outcome[...] = jnp.zeros(outcome.shape, F32)
        for i in range(cont_count):
            for s in range(sources):

                @pl.when(source_ref[i] == s)
                def _():
                    pltpu.make_async_copy(piece_refs[s].at[place_ref[i]], cache.at[i], sem.at[i]).start()

        for i in range(cont_count):
            pltpu.make_async_copy(piece_refs[0].at[0], cache.at[i], sem.at[i]).wait()

    base = kv_here * pref_len
    pick_row = lax.broadcasted_iota(jnp.int32, (heads_here, chunk), 0)
    pick_col = lax.broadcasted_iota(jnp.int32, (heads_here, chunk), 1)
    parts = [None] * (cols // chunk)
    for k in range(kv_here):
        keys = cache[c, k * pref_len : (k + 1) * pref_len, :]
        pick = (pick_row == pick_col % group + k * group).astype(F32).astype(BF16)
        read = dot_tn(cache[c, base : base + heads_here, :], pick) + dot_tn(
            cache[c, base + heads_here : base + 2 * heads_here, :], pick
        )
        for n in range(cols // chunk):
            start = n * chunk
            first = start // group
            query = query_ref[0, first : first + span, k * group : (k + 1) * group, :].reshape(chunk, head_dim)
            scores = dot_nt(keys, query)
            own_top = stat_ref[0, 3 * k : 3 * k + 1, start : start + chunk]
            own_total = stat_ref[0, 3 * k + 1 : 3 * k + 2, start : start + chunk]
            own_sum = stat_ref[0, 3 * k + 2 : 3 * k + 3, start : start + chunk]
            top = jnp.maximum(jnp.max(scores, axis=0, keepdims=True), own_top)
            expo = jnp.exp2((scores - top) * factor)
            shrink = jnp.exp2((own_top - top) * factor)
            total = jnp.sum(expo, axis=0, keepdims=True) + own_total * shrink
            summed = jnp.sum(expo * read, axis=0, keepdims=True) + own_sum * shrink
            value = summed / total
            parts[n] = value if parts[n] is None else parts[n] + value
    for n in range(cols // chunk):
        outcome[pl.ds(c, 1), n * chunk : (n + 1) * chunk] = parts[n]

    @pl.when(c == cont_count - 1)
    def _():
        values = outcome[...]
        where_row = lax.broadcasted_iota(jnp.int32, (cols, clen), 0)
        where_col = lax.broadcasted_iota(jnp.int32, (cols, clen), 1)
        fold = (where_row // group == where_col).astype(F32).astype(BF16)
        high = values.astype(BF16).astype(F32)
        middle = (values - high).astype(BF16).astype(F32)
        low = values - high - middle
        stacked = jnp.concatenate([high, middle, low], axis=0).astype(BF16)
        folded = lax.dot_general(stacked, fold, (((1,), (0,)), ((), ())), preferred_element_type=F32)
        rows = outcome.shape[0]
        token = folded[:rows] + folded[rows : 2 * rows] + folded[2 * rows :]
        out_ref[0 : token.shape[0], :] = token
        lane = lax.broadcasted_iota(jnp.int32, (1, clen), 1)
        spot_rows = out_ref.shape[0] - rows
        spot = lax.broadcasted_iota(jnp.int32, (spot_rows, clen), 0) * clen + lax.broadcasted_iota(
            jnp.int32, (spot_rows, clen), 1
        )
        term = jnp.zeros((spot_rows, clen), F32)
        for i in range(cont_count):
            kept = jnp.where(lane < length_ref[i], token[i : i + 1], 0.0)
            choice = jnp.sum(kept, axis=1, keepdims=True)
            term = term + jnp.where(spot == target_ref[i], choice, 0.0)
        out_ref[rows:, :] = term


def shift(x, axis, by, size):
    return lax.ppermute(x, axis, [(i, (i + by) % size) for i in range(size)])


def swap(x, axis, bit, size):
    return lax.ppermute(x, axis, [(i, i ^ bit) for i in range(size)])


def exchange_sum(x, axis, size):
    if size > DIRECT_LIMIT:
        return lax.psum(x, axis)
    return x + sum(shift(x, axis, by, size) for by in range(1, size))


def doubling_sum(x, axis, size):
    if size & (size - 1):
        return lax.psum(x, axis)
    bit = 1
    while bit < size:
        x = x + swap(x, axis, bit, size)
        bit *= 2
    return x


def per_device(mesh_shape, *args):
    (cont_queries, cont_keys, cont_values, prefix_kv, probe, question_row, cont_slot, cont_length, gold) = args
    wide, narrow = mesh_shape["wide"], mesh_shape["narrow"]
    cont_count, clen, heads_here, head_dim = cont_queries.shape
    kv_here = cont_keys.shape[2]
    group = heads_here // kv_here
    cols = clen * group
    quest_here, _, pref_len = prefix_kv.shape[:3]
    questions = question_row.shape[0]
    packed_rows = kv_here * pref_len + 2 * heads_here

    packed = pl.pallas_call(
        pack_kernel,
        grid=(quest_here,),
        in_specs=[
            pl.BlockSpec((1, 2, pref_len, kv_here, head_dim), lambda i: (i, 0, 0, 0, 0)),
            pl.BlockSpec((heads_here, head_dim), lambda i: (0, 0)),
        ],
        out_specs=pl.BlockSpec((1, packed_rows, head_dim), lambda i: (i, 0, 0)),
        out_shape=jax.ShapeDtypeStruct((quest_here, packed_rows, head_dim), BF16),
        name="pack",
    )(prefix_kv, probe)

    wanted = question_row[cont_slot // ANSWERS].astype(jnp.int32)
    me = lax.axis_index("wide")
    if wide <= DIRECT_LIMIT:
        pieces = [packed] + [shift(packed, "wide", by, wide) for by in range(1, wide)]
        source = (me - wanted // quest_here) % wide
        place = wanted % quest_here
    else:
        pieces = [lax.all_gather(packed, "wide", axis=0, tiled=True)]
        source = jnp.zeros_like(wanted)
        place = wanted

    stat_rows = 3 * kv_here
    stats = pl.pallas_call(
        own_kernel,
        grid=(cont_count,),
        in_specs=[
            pl.BlockSpec((1, clen, heads_here, head_dim), lambda i: (i, 0, 0, 0)),
            pl.BlockSpec((1, clen, kv_here, head_dim), lambda i: (i, 0, 0, 0)),
            pl.BlockSpec((1, clen, kv_here, head_dim), lambda i: (i, 0, 0, 0)),
            pl.BlockSpec((heads_here, head_dim), lambda i: (0, 0)),
        ],
        out_specs=pl.BlockSpec((1, stat_rows, cols), lambda i: (i, 0, 0)),
        out_shape=jax.ShapeDtypeStruct((cont_count, stat_rows, cols), F32),
        cost_estimate=pl.CostEstimate(flops=10**9, bytes_accessed=3 * 10**6, transcendentals=10**6),
        name="own",
    )(cont_queries, cont_keys, cont_values, probe)

    target = wanted * ANSWERS + cont_slot % ANSWERS
    spot_rows = -(-questions * ANSWERS // clen)
    rows = -(-cont_count // 8) * 8
    payload = pl.pallas_call(
        lambda *refs: prefix_kernel(*refs, sources=len(pieces)),
        grid_spec=pltpu.PrefetchScalarGridSpec(
            num_scalar_prefetch=4,
            grid=(cont_count,),
            in_specs=[
                pl.BlockSpec((1, clen, heads_here, head_dim), lambda i, *_: (i, 0, 0, 0)),
                pl.BlockSpec((1, stat_rows, cols), lambda i, *_: (i, 0, 0)),
            ]
            + [pl.BlockSpec(memory_space=pl.ANY)] * len(pieces),
            out_specs=pl.BlockSpec((rows + 8 * (-(-spot_rows // 8)), clen), lambda i, *_: (0, 0)),
            scratch_shapes=[
                pltpu.VMEM((cont_count, packed_rows, head_dim), BF16),
                pltpu.VMEM((rows, cols), F32),
                pltpu.SemaphoreType.DMA((cont_count,)),
            ],
        ),
        out_shape=jax.ShapeDtypeStruct((rows + 8 * (-(-spot_rows // 8)), clen), F32),
        name="prefix",
    )(source, place, target, cont_length, cont_queries, stats, *pieces)

    summed = exchange_sum(payload, "narrow", narrow)
    token_score = summed[:cont_count]
    totals = doubling_sum(summed[rows : rows + spot_rows], "wide", wide)
    totals = totals.reshape(-1)[: questions * ANSWERS].reshape(questions, ANSWERS)
    first_row = me * quest_here
    owned = lax.dynamic_slice_in_dim(totals, first_row, quest_here, 0)
    logprob = owned - jax.nn.logsumexp(owned, axis=1, keepdims=True)
    owned_rows = first_row + jnp.arange(quest_here, dtype=jnp.int32)
    matches = question_row[None, :] == owned_rows[:, None]
    gold_owned = jnp.sum(jnp.where(matches, gold[None, :], 0), axis=1)
    answer_ids = jnp.arange(ANSWERS, dtype=jnp.int32)[None, :]
    owned_loss = -jnp.sum(jnp.where(answer_ids == gold_owned[:, None], logprob, 0.0), axis=1)
    return (token_score, logprob, owned_loss)


def solution(mesh):
    shape = dict(mesh.shape)
    return jax.shard_map(
        lambda *args: per_device(shape, *args),
        mesh=mesh,
        in_specs=(
            P(("groups", "wide"), None, "narrow", None),
            P(("groups", "wide"), None, "narrow", None),
            P(("groups", "wide"), None, "narrow", None),
            P(("groups", "wide"), None, None, "narrow", None),
            P("narrow", None),
            P("groups"),
            P(("groups", "wide")),
            P(("groups", "wide")),
            P("groups"),
        ),
        out_specs=(P(("groups", "wide"), None), P(("groups", "wide"), None), P(("groups", "wide"))),
        check_vma=False,
    )
```

```python
import math

import jax
import jax.numpy as jnp
from jax import lax
from jax.experimental import pallas as pl
from jax.experimental.pallas import tpu as pltpu
from jax.sharding import PartitionSpec as P

ANSWERS = 4
DIRECT_LIMIT = 8
KERNEL_BYTES = 16 << 20
F32 = jnp.float32
BF16 = jnp.bfloat16


def dot_nt(a, b):
    return lax.dot_general(a, b, (((1,), (1,)), ((), ())), preferred_element_type=F32)


def dot_tn(a, b):
    return lax.dot_general(a, b, (((0,), (0,)), ((), ())), preferred_element_type=F32)


def split_heads(joined):
    rows, heads, depth = joined.shape
    flat = joined.reshape(rows * heads, depth)
    to = lax.broadcasted_iota(jnp.int32, (rows, rows * heads), 0)
    at = lax.broadcasted_iota(jnp.int32, (rows, rows * heads), 1)
    return [
        lax.dot_general(
            (at == to * heads + k).astype(F32).astype(BF16),
            flat,
            (((1,), (0,)), ((), ())),
            preferred_element_type=F32,
        ).astype(BF16)
        for k in range(heads)
    ]


def column_chunk(clen, group_size):
    cols = clen * group_size
    return 256 if cols % 256 == 0 else cols


def pack_kernel(prefix_ref, probe_ref, *refs):
    count = (len(refs) - 2) // 2
    moved, out_ref, kept, sem = refs[:count], refs[count], refs[count + 1 : -1], refs[-1]
    copies = [pltpu.make_async_copy(moved[i], kept[i], sem.at[i]) for i in range(count)]
    for copy in copies:
        copy.start()
    quest_here, _, pref_len, kv_here, head_dim = prefix_ref.shape
    heads_here = probe_ref.shape[0]
    group = heads_here // kv_here
    base = kv_here * pref_len

    def body(i, carry):
        reads = []
        keys, values = split_heads(prefix_ref[i, 0]), split_heads(prefix_ref[i, 1])
        for k in range(kv_here):
            out_ref[i, k * pref_len : (k + 1) * pref_len, :] = keys[k]
            reads.append(dot_nt(probe_ref[k * group : (k + 1) * group, :], values[k]))
        read = jnp.concatenate(reads, axis=0)
        high = read.astype(BF16)
        low = (read - high.astype(F32)).astype(BF16)
        out_ref[i, base : base + heads_here, :] = high
        out_ref[i, base + heads_here : base + 2 * heads_here, :] = low
        return carry

    lax.fori_loop(0, quest_here, body, 0)
    for copy in copies:
        copy.wait()


def own_kernel(query_ref, key_ref, value_ref, probe_ref, stat_ref):
    cont_count, clen, kv_here, head_dim = key_ref.shape
    group = query_ref.shape[2] // kv_here
    cols = clen * group
    chunk = column_chunk(clen, group)
    span = chunk // group
    factor = math.log2(math.e) / math.sqrt(head_dim)
    row = lax.broadcasted_iota(jnp.int32, (span, chunk), 0)
    col = lax.broadcasted_iota(jnp.int32, (span, chunk), 1)
    seen = row * group <= col

    def body(c, carry):
        all_keys, all_values = split_heads(key_ref[c]), split_heads(value_ref[c])
        for k in range(kv_here):
            keys = all_keys[k]
            probe = probe_ref[k * group : (k + 1) * group, :]
            read = dot_nt(all_values[k], jnp.concatenate([probe] * (chunk // group), axis=0))
            for start in range(0, cols, chunk):
                first = start // group
                last = first + span
                query = query_ref[c, first:last, k * group : (k + 1) * group, :].reshape(chunk, head_dim)
                scores = dot_nt(keys[:last], query)
                edge = jnp.where(seen, scores[first:last], -jnp.inf)
                scores = edge if first == 0 else jnp.concatenate([scores[:first], edge], axis=0)
                top = jnp.max(scores, axis=0, keepdims=True)
                expo = jnp.exp2((scores - top) * factor)
                total = jnp.sum(expo, axis=0, keepdims=True)
                summed = jnp.sum(expo * read[:last], axis=0, keepdims=True)
                stat_ref[c, 3 * k : 3 * k + 1, start : start + chunk] = top
                stat_ref[c, 3 * k + 1 : 3 * k + 2, start : start + chunk] = total
                stat_ref[c, 3 * k + 2 : 3 * k + 3, start : start + chunk] = summed
        return carry

    lax.fori_loop(0, cont_count, body, 0)


def prefix_kernel(question_ref, slot_ref, length_ref, query_ref, stat_ref, *rest, wide, quest_here):
    piece_refs, (out_ref, cache, outcome) = rest[:-3], rest[-3:]
    sources = len(piece_refs)
    cont_count, clen, heads_here, head_dim = query_ref.shape
    kv_here = stat_ref.shape[1] // 3
    group = heads_here // kv_here
    cols = clen * group
    chunk = column_chunk(clen, group)
    span = chunk // group
    pref_len = (cache.shape[0] - 2 * heads_here) // kv_here
    factor = math.log2(math.e) / math.sqrt(head_dim)
    me = lax.axis_index("wide")
    outcome[...] = jnp.zeros(outcome.shape, F32)
    base = kv_here * pref_len
    pick_row = lax.broadcasted_iota(jnp.int32, (heads_here, chunk), 0)
    pick_col = lax.broadcasted_iota(jnp.int32, (heads_here, chunk), 1)
    picks = [
        (pick_row == lax.rem(pick_col, group) + k * group).astype(F32).astype(BF16) for k in range(kv_here)
    ]

    def row_of(c):
        return question_ref[lax.div(slot_ref[c], ANSWERS)]

    def body(c, carry):
        wanted = row_of(c)
        if sources == 1:
            pltpu.sync_copy(piece_refs[0].at[wanted], cache)
        else:
            source = lax.rem(me - lax.div(wanted, quest_here) + wide, wide)
            for s in range(sources):

                @pl.when(source == s)
                def _():
                    cache[...] = piece_refs[s][lax.rem(wanted, quest_here)]

        parts = [None] * (cols // chunk)
        for k in range(kv_here):
            keys = cache[k * pref_len : (k + 1) * pref_len, :]
            read = dot_tn(cache[base : base + heads_here, :], picks[k]) + dot_tn(
                cache[base + heads_here : base + 2 * heads_here, :], picks[k]
            )
            for n in range(cols // chunk):
                start = n * chunk
                first = start // group
                query = query_ref[c, first : first + span, k * group : (k + 1) * group, :].reshape(chunk, head_dim)
                scores = dot_nt(keys, query)
                own_top = stat_ref[c, 3 * k : 3 * k + 1, start : start + chunk]
                own_total = stat_ref[c, 3 * k + 1 : 3 * k + 2, start : start + chunk]
                own_sum = stat_ref[c, 3 * k + 2 : 3 * k + 3, start : start + chunk]
                top = jnp.maximum(jnp.max(scores, axis=0, keepdims=True), own_top)
                expo = jnp.exp2((scores - top) * factor)
                shrink = jnp.exp2((own_top - top) * factor)
                total = jnp.sum(expo, axis=0, keepdims=True) + own_total * shrink
                summed = jnp.sum(expo * read, axis=0, keepdims=True) + own_sum * shrink
                value = summed / total
                parts[n] = value if parts[n] is None else parts[n] + value
        for n in range(cols // chunk):
            outcome[pl.ds(c, 1), n * chunk : (n + 1) * chunk] = parts[n]
        return carry

    lax.fori_loop(0, cont_count, body, 0)
    values = outcome[...]
    where_row = lax.broadcasted_iota(jnp.int32, (cols, clen), 0)
    where_col = lax.broadcasted_iota(jnp.int32, (cols, clen), 1)
    fold = (lax.div(where_row, group) == where_col).astype(F32).astype(BF16)
    high = values.astype(BF16).astype(F32)
    middle = (values - high).astype(BF16).astype(F32)
    low = values - high - middle
    stacked = jnp.concatenate([high, middle, low], axis=0).astype(BF16)
    folded = lax.dot_general(stacked, fold, (((1,), (0,)), ((), ())), preferred_element_type=F32)
    rows = outcome.shape[0]
    token = folded[:rows] + folded[rows : 2 * rows] + folded[2 * rows :]
    out_ref[0:rows, :] = token
    lane = lax.broadcasted_iota(jnp.int32, (1, clen), 1)
    spot = spots(out_ref.shape[0] - rows, clen)
    term = jnp.zeros(spot.shape, F32)
    for i in range(cont_count):
        kept = jnp.where(lane < length_ref[i], token[i : i + 1], 0.0)
        choice = jnp.sum(kept, axis=1, keepdims=True)
        target = row_of(i) * ANSWERS + lax.rem(slot_ref[i], ANSWERS)
        term = term + jnp.where(spot == target, choice, 0.0)
    out_ref[rows:, :] = term


def spots(rows, width):
    return lax.broadcasted_iota(jnp.int32, (rows, width), 0) * width + lax.broadcasted_iota(
        jnp.int32, (rows, width), 1
    )


def final_kernel(question_ref, gold_ref, mine_ref, other_ref, near_ref, far_ref, token_ref, logprob_ref, loss_ref):
    cont_count = token_ref.shape[0]
    token_ref[...] = mine_ref[:cont_count, :] + other_ref[:cont_count, :]
    totals = near_ref[...] + far_ref[...]
    quest_here = logprob_ref.shape[0]
    first_row = lax.axis_index("wide") * quest_here
    spot = spots(*totals.shape)
    column = lax.broadcasted_iota(jnp.int32, (1, ANSWERS), 1)

    def total_of(x):
        return jnp.sum(jnp.sum(x, axis=0, keepdims=True), axis=1, keepdims=True)

    for r in range(quest_here):
        row = first_row + r
        shown = (spot >= row * ANSWERS) & (spot < (row + 1) * ANSWERS)
        scores = jnp.where(shown, totals, -jnp.inf)
        top = jnp.max(jnp.max(scores, axis=0, keepdims=True), axis=1, keepdims=True)
        logs = jnp.where(shown, totals - (top + jnp.log(total_of(jnp.exp(scores - top)))), 0.0)
        gold = jnp.int32(0)
        for q in range(question_ref.shape[0]):
            gold = gold + jnp.where(question_ref[q] == row, gold_ref[q], 0)
        line = jnp.zeros((1, ANSWERS), F32)
        for a in range(ANSWERS):
            line = line + jnp.where(column == a, total_of(jnp.where(spot == row * ANSWERS + a, logs, 0.0)), 0.0)
        logprob_ref[r : r + 1, :] = line
        loss_ref[r] = -jnp.sum(jnp.where(spot == row * ANSWERS + gold, logs, 0.0))


def shift(x, axis, by, size):
    return lax.ppermute(x, axis, [(i, (i + by) % size) for i in range(size)])


def swap(x, bit_wide, bit_narrow, wide, narrow):
    pairs = [
        (w * narrow + n, (w ^ bit_wide) * narrow + (n ^ bit_narrow)) for w in range(wide) for n in range(narrow)
    ]
    return lax.ppermute(x, ("wide", "narrow"), pairs)


def in_hbm(x):
    return pltpu.with_memory_space_constraint(x, pltpu.HBM)


def in_vmem(x):
    return pltpu.with_memory_space_constraint(x, pltpu.VMEM)


def per_device(mesh_shape, *args):
    (cont_queries, cont_keys, cont_values, prefix_kv, probe, question_row, cont_slot, cont_length, gold) = args
    wide, narrow = mesh_shape["wide"], mesh_shape["narrow"]
    cont_count, clen, heads_here, head_dim = cont_queries.shape
    kv_here = cont_keys.shape[2]
    group = heads_here // kv_here
    cols = clen * group
    quest_here, _, pref_len = prefix_kv.shape[:3]
    questions = question_row.shape[0]
    packed_rows = kv_here * pref_len + 2 * heads_here

    whole = pl.BlockSpec(memory_space=pltpu.VMEM)
    scalars = pl.BlockSpec(memory_space=pltpu.SMEM)
    outside = pl.BlockSpec(memory_space=pltpu.HBM)
    moved = [in_hbm(x) for x in (cont_queries, cont_keys, cont_values)]
    packed, queries, keys, values = pl.pallas_call(
        pack_kernel,
        in_specs=[whole] * 2 + [outside] * len(moved),
        out_specs=(whole,) * (1 + len(moved)),
        out_shape=(
            jax.ShapeDtypeStruct((quest_here, packed_rows, head_dim), BF16),
            *[pltpu.VMEM(x.shape, x.dtype) for x in moved],
        ),
        scratch_shapes=[pltpu.SemaphoreType.DMA((len(moved),))],
        compiler_params=pltpu.CompilerParams(vmem_limit_bytes=KERNEL_BYTES),
        name="pack",
    )(in_hbm(prefix_kv), in_hbm(probe), *moved)

    if wide <= DIRECT_LIMIT:
        pieces = [packed] + [shift(packed, "wide", by, wide) for by in range(1, wide)]
    else:
        pieces = [lax.all_gather(packed, "wide", axis=0, tiled=True)]
    direct = len(pieces) > 1

    queries = in_vmem(queries)
    stats = pl.pallas_call(
        own_kernel,
        in_specs=[whole] * 4,
        out_specs=whole,
        out_shape=pltpu.VMEM((cont_count, 3 * kv_here, cols), F32),
        cost_estimate=pl.CostEstimate(flops=10**9, bytes_accessed=3 * 10**6, transcendentals=10**6),
        compiler_params=pltpu.CompilerParams(vmem_limit_bytes=KERNEL_BYTES),
        name="own",
    )(queries, in_vmem(keys), in_vmem(values), in_hbm(probe))

    spot_rows = 8 * -(-questions * ANSWERS // (8 * clen))
    rows = 8 * -(-cont_count // 8)
    payload = pl.pallas_call(
        lambda *refs: prefix_kernel(*refs, wide=wide, quest_here=quest_here),
        in_specs=[scalars] * 3 + [whole] * 2 + [whole if direct else outside] * len(pieces),
        out_specs=whole,
        scratch_shapes=[pltpu.VMEM((packed_rows, head_dim), BF16), pltpu.VMEM((rows, cols), F32)],
        out_shape=pltpu.VMEM((rows + spot_rows, clen), F32),
        compiler_params=pltpu.CompilerParams(vmem_limit_bytes=KERNEL_BYTES),
        name="prefix",
    )(question_row, cont_slot, cont_length, in_vmem(queries), in_vmem(stats), *([in_vmem(x) for x in pieces] if direct else pieces))

    mine = payload
    bit = 1
    while 2 * bit < narrow:
        mine = mine + swap(mine, 0, bit, wide, narrow)
        bit *= 2
    other = swap(mine, 0, bit, wide, narrow)
    beside = swap(mine[rows:], 1, 0, wide, narrow)
    across = swap(mine[rows:], 1, bit, wide, narrow)
    near = mine[rows:] + other[rows:] + (beside + across)
    far = jnp.zeros_like(near)
    bit = 2
    while bit < wide:
        near = near + far
        far = swap(near, bit, 0, wide, narrow)
        bit *= 2
    token_score, logprob, owned_loss = pl.pallas_call(
        final_kernel,
        in_specs=[scalars] * 2 + [whole] * 4,
        out_specs=(whole, whole, scalars),
        out_shape=(
            jax.ShapeDtypeStruct((cont_count, clen), F32),
            jax.ShapeDtypeStruct((quest_here, ANSWERS), F32),
            jax.ShapeDtypeStruct((quest_here,), F32),
        ),
        compiler_params=pltpu.CompilerParams(vmem_limit_bytes=KERNEL_BYTES),
        name="final",
    )(question_row, gold, in_vmem(mine), in_vmem(other), in_vmem(near), in_vmem(far))
    return (token_score, logprob, owned_loss)


def solution(mesh):
    shape = dict(mesh.shape)
    if any(size < 2 or size & (size - 1) for size in (shape["wide"], shape["narrow"])):
        raise ValueError("axis size")
    return jax.shard_map(
        lambda *args: per_device(shape, *args),
        mesh=mesh,
        in_specs=(
            P(("groups", "wide"), None, "narrow", None),
            P(("groups", "wide"), None, "narrow", None),
            P(("groups", "wide"), None, "narrow", None),
            P(("groups", "wide"), None, None, "narrow", None),
            P("narrow", None),
            P("groups"),
            P(("groups", "wide")),
            P(("groups", "wide")),
            P("groups"),
        ),
        out_specs=(P(("groups", "wide"), None), P(("groups", "wide"), None), P(("groups", "wide"))),
        check_vma=False,
    )
```
